32 devices in a mesh: ctx: 16 (over z, x, core), tp: 2 (over y).
Axes of the slice: x: 2, y: 2, z: 4, core: 2. Of those that a mesh axis runs over, the one named last changes fastest.
Arguments:
- queries: bfloat16 [4096, 8192], P('ctx', 'tp'), may hold values from -6 to 6
- keys: bfloat16 [4096, 1024], P('ctx', 'tp'), may hold values from -6 to 6
- values: bfloat16 [4096, 1024], P('ctx', 'tp'), may hold values from -6 to 6
- documents: int32 [4096], replicated, may hold values from 0 to 3, never falling along the last dimension, each value on 1 to 2048 neighbouring positions
- hist_q: float32 [16, 64], P(None, 'tp'), may hold values from 0.75 to 5.4
- hist_kv: float32 [2, 16, 8], P(None, None, 'tp'), may hold values from 0.75 to 5.4
- out_weight: bfloat16 [8192, 8192], P(('tp', 'ctx')), may hold values from -0.0625 to 0.0625
Outputs:
- mixed: bfloat16 [4096, 8192], P('ctx', 'tp')
- new_hist_q: float32 [16, 64], P(None, 'tp')
- new_hist_kv: float32 [2, 16, 8], P(None, None, 'tp')
The draws below stay inside these ranges and needn't reach their ends.
All inputs are finite; a program needn't handle non-finite values.
Results may differ from the reference program's by a relative error of at most 0.015.
Values may be sent and summed in bfloat16 or wider, within the bound.
A program may use at most 192 MiB of HBM per device.

```python
import math
import jax
import jax.numpy as jnp
import numpy as np
from jax import lax

D = 8192
HEADS = 64
KV = 8
HD = 128
HIST = 16
SEQ = 4096


def drawn_pair(key):
    base = jax.random.fold_in(key, 4417)
    first, second = jax.random.split(base, 2)
    query_part = jnp.clip(jax.random.normal(first, (SEQ, HEADS, HD), jnp.float32), -6.0, 6.0)
    key_part = jnp.clip(jax.random.normal(second, (SEQ, KV, HD), jnp.float32), -6.0, 6.0)
    return (query_part.reshape(SEQ, HEADS * HD), key_part.reshape(SEQ, KV * HD))


def draw_queries(key, part):
    return drawn_pair(key)[0].astype(jnp.bfloat16)


def draw_keys(key, part):
    return drawn_pair(key)[1].astype(jnp.bfloat16)


def history(key, leading, count):
    base = jax.random.fold_in(key, 9173)
    first, second, third = jax.random.split(base, 3)
    lowest, highest, peak_lowest, peak_highest = (0.75, 1.8, 1.8, 2.4)
    spread = jax.random.uniform(first, (leading, HIST, count), jnp.float32, math.log(lowest), math.log(highest))
    entries = jnp.exp(spread)
    peaks = jax.random.uniform(second, (leading, 1, count), jnp.float32, peak_lowest, peak_highest)
    peak_slot = jax.random.randint(third, (leading, 1, count), 0, HIST)
    slots = jnp.arange(HIST, dtype=jnp.int32)[None, :, None]
    return jnp.where(slots == peak_slot, peaks, entries)


def draw_hist_q(key, part):
    return history(jax.random.fold_in(key, 31), 1, HEADS)[0]


def draw_hist_kv(key, part):
    return history(jax.random.fold_in(key, 57), 2, KV)


def steps_of(stream_key, shape, cuts, least, high):
    factor_of = 1.0
    for axis_at, blocks in cuts:
        draws = jax.random.uniform(jax.random.fold_in(jax.random.fold_in(stream_key, 6), axis_at), (blocks,), jnp.float32, least / len(cuts), high / len(cuts))
        factor_of = factor_of * jnp.repeat(jnp.exp(draws), shape[axis_at] // blocks).reshape((-1,) + (1,) * (len(shape) - 1 - axis_at))
    return factor_of


def length_profile(count, total, bound, skew):
    weights = [(1 << 20) // math.isqrt(standing ** skew) + 1 for standing in range(2, count + 1)]
    spare, counts = total - bound - (count - 1), [1] * (count - 1)
    while spare > 0:
        movable = [i for i in range(count - 1) if counts[i] < bound]
        pool, remaining = sum([weights[i] for i in movable]), spare
        for i in movable:
            addition = min(bound - counts[i], max(1, remaining * weights[i] // pool), spare)
            counts[i] = counts[i] + addition
            spare = spare - addition
    return np.array([bound] + counts)


def uneven_parts(rng, count, total, bound, slope):
    if count == 2:
        one = jax.random.randint(rng, (), max(1, total - bound), min(bound, total - 1) + 1)
        return jnp.stack([one, total - one])
    sizes = jnp.asarray(length_profile(count, total, bound, slope), jnp.int32)
    couples = (count - 1) // 2
    donor, sink = sizes[1:1 + 2 * couples:2], sizes[2:2 + 2 * couples:2]
    room = jnp.minimum(donor - 1, bound - sink)
    shifted = jax.random.randint(jax.random.fold_in(rng, 1), (couples,), 0, 1 << 20) % (room + 1)
    sizes = sizes.at[1:1 + 2 * couples:2].set(donor - shifted).at[2:2 + 2 * couples:2].set(sink + shifted)
    return sizes[jax.random.permutation(jax.random.fold_in(rng, 2), count)]


def centred(stream_key, shape, scale, limit, cuts=(), kind=jnp.bfloat16):
    drawn = scale * jax.random.normal(stream_key, shape, jnp.float32)
    if cuts:
        drawn = drawn * steps_of(stream_key, shape, cuts, -0.22, 0.18)
    return jnp.clip(drawn, -limit, limit).astype(kind)


def setup_inputs(seed: int = 0) -> dict:
    arg_keys = jax.random.split(jax.random.key(seed), 8)
    return {
        "queries": draw_queries(jax.random.fold_in(arg_keys[7], 71), 0),
        "keys": draw_keys(jax.random.fold_in(arg_keys[7], 71), 0),
        "values": centred(arg_keys[2], (SEQ, KV * HD), 1.0, 6.0, ((0, 16), (1, 2))),
        "documents": jnp.searchsorted(jnp.cumsum(uneven_parts(arg_keys[3], 4, SEQ, SEQ // 2, 0)), jnp.arange(SEQ), side="right").astype(jnp.int32),
        "hist_q": draw_hist_q(jax.random.fold_in(arg_keys[7], 71), 0),
        "hist_kv": draw_hist_kv(jax.random.fold_in(arg_keys[7], 71), 0),
        "out_weight": centred(arg_keys[6], (HEADS * HD, D), (HEADS * HD) ** -0.5, 0.0625, ((0, 32),)),
    }


def reference(queries, keys, values, documents, hist_q, hist_kv, out_weight):
    group = HEADS // KV
    lim_q = lax.optimization_barrier(jnp.max(hist_q, axis=0)).reshape(KV, group)
    lim_kv = lax.optimization_barrier(jnp.max(hist_kv, axis=1))
    raw_q = queries.astype(jnp.float32).reshape(SEQ, KV, group, HD)
    qc = jnp.clip(raw_q, -lim_q[None, :, :, None], lim_q[None, :, :, None]).astype(jnp.bfloat16)
    raw_k = keys.astype(jnp.float32).reshape(SEQ, KV, HD)
    raw_v = values.astype(jnp.float32).reshape(SEQ, KV, HD)
    kc = jnp.clip(raw_k, -lim_kv[0][None, :, None], lim_kv[0][None, :, None]).astype(jnp.bfloat16)
    vc = jnp.clip(raw_v, -lim_kv[1][None, :, None], lim_kv[1][None, :, None]).astype(jnp.bfloat16)
    scale = 1.0 / math.sqrt(HD)
    positions = jnp.arange(SEQ, dtype=jnp.int32)
    blk = min(512, SEQ)
    pieces = []
    for number in range(SEQ // blk):
        first = number * blk
        last = first + blk
        allowed = (positions[:last][None, :] <= positions[first:last][:, None]) & (documents[:last][None, :] == documents[first:last][:, None])

        def one_head(args):
            q_head, k_head, v_head = args
            scores = jnp.einsum('tjd,bd->jtb', q_head.astype(jnp.float32), k_head.astype(jnp.float32)) * scale
            top = lax.optimization_barrier(jnp.max(jnp.where(allowed[None], scores, -1e+30), axis=-1))
            weights = jnp.where(allowed[None], jnp.exp(scores - top[..., None]), 0.0)
            total = lax.optimization_barrier(jnp.sum(weights, axis=-1))
            mixed_v = jnp.einsum('jtb,bd->jtd', weights.astype(jnp.bfloat16).astype(jnp.float32), v_head.astype(jnp.float32))
            return mixed_v / total[..., None]
        heads_out = lax.map(one_head, (jnp.transpose(qc[first:last], (1, 0, 2, 3)), jnp.transpose(kc[:last], (1, 0, 2)), jnp.transpose(vc[:last], (1, 0, 2))))
        pieces.append(jnp.transpose(heads_out, (2, 0, 1, 3)).reshape(blk, HEADS * HD))
    attn = jnp.concatenate(pieces, axis=0).astype(jnp.bfloat16)
    mixed = jnp.dot(attn, out_weight, preferred_element_type=jnp.float32).astype(jnp.bfloat16)
    cur_q = lax.optimization_barrier(jnp.max(jnp.abs(raw_q.reshape(SEQ, HEADS, HD)), axis=(0, 2)))
    cur_kv = jnp.stack([lax.optimization_barrier(jnp.max(jnp.abs(raw_k), axis=(0, 2))), lax.optimization_barrier(jnp.max(jnp.abs(raw_v), axis=(0, 2)))])
    new_hist_q = jnp.concatenate([cur_q[None], hist_q[:-1]], axis=0)
    new_hist_kv = jnp.concatenate([cur_kv[:, None], hist_kv[:, :-1]], axis=1)
    return (mixed, new_hist_q, new_hist_kv)
```

```python
import functools
import math

import jax
import jax.numpy as jnp
from jax import lax
from jax.experimental import pallas as pl
from jax.experimental.pallas import tpu as pltpu
from jax.sharding import PartitionSpec as P

NEG = -1e30


def attend_kernel(
    low_ref, high_ref, base_ref, q_ref, k_ref, v_ref, start_ref, o_ref, acc_ref, top_ref,
    *, stacks, stack, head_size, block, scale
):
    number = pl.program_id(0)
    rows = q_ref.shape[1]
    tall = stack * rows
    row_pos = base_ref[number] + lax.broadcasted_iota(jnp.int32, (rows, block), 0)
    row_start = start_ref[0]
    acc_ref[...] = jnp.zeros_like(acc_ref)
    top_ref[...] = jnp.full_like(top_ref, NEG)
    queries = []
    for part in range(stacks):
        heads = [
            q_ref[0, :, (part * stack + j) * head_size : (part * stack + j + 1) * head_size]
            for j in range(stack)
        ]
        queries.append(jnp.concatenate(heads, axis=0))

    def step(key_number, carry):
        key_first = pl.multiple_of(key_number * block, block)
        keys = k_ref[pl.ds(key_first, block), :]
        values = v_ref[pl.ds(key_first, block), :]
        key_pos = key_first + lax.broadcasted_iota(jnp.int32, (rows, block), 1)
        bias = jnp.where((key_pos <= row_pos) & (key_pos >= row_start), 0.0, NEG)
        for part in range(stacks):
            scores = lax.dot_general(
                queries[part], keys, (((1,), (1,)), ((), ())), preferred_element_type=jnp.float32
            )
            scores = (scores.reshape(stack, rows, block) * scale + bias[None]).reshape(tall, block)
            old_top = top_ref[part]
            top = jnp.maximum(old_top, jnp.max(scores, axis=1, keepdims=True))
            weights = jnp.exp2(scores - top[:, :1]).astype(jnp.bfloat16)
            decay = jnp.exp2(old_top - top)
            top_ref[part] = top
            product = jnp.dot(weights, values, preferred_element_type=jnp.float32)
            acc_ref[part] = acc_ref[part] * jnp.concatenate([decay, decay], axis=1) + product
        return carry

    lax.fori_loop(low_ref[number], high_ref[number], step, 0)
    for part in range(stacks):
        result = acc_ref[part, :, :head_size] / acc_ref[part, :, head_size:]
        for j in range(stack):
            first = (part * stack + j) * head_size
            o_ref[0, :, first : first + head_size] = result[j * rows : (j + 1) * rows].astype(
                o_ref.dtype
            )


def attend(queries, keys, values, starts, bases, chunk, rows, head_size):
    groups, _, width = queries.shape
    heads = width // head_size
    stack = math.gcd(heads, 4)
    stacks = math.gcd(heads // stack, 2)
    per_step = stack * stacks
    tokens = keys.shape[0]
    block = math.gcd(tokens, 512)
    low = starts[:, 0, 0] // block
    high = (bases + rows - 1) // block + 1
    kernel = functools.partial(
        attend_kernel, stacks=stacks, stack=stack, head_size=head_size, block=block,
        scale=math.log2(math.e) / math.sqrt(head_size),
    )
    spec = pltpu.PrefetchScalarGridSpec(
        num_scalar_prefetch=3,
        grid=(groups, heads // per_step),
        in_specs=[
            pl.BlockSpec((1, rows, per_step * head_size), lambda g, h, *_: (g, chunk, h)),
            pl.BlockSpec((tokens, head_size), lambda g, h, *_: (0, 0)),
            pl.BlockSpec((tokens, 2 * head_size), lambda g, h, *_: (0, 0)),
            pl.BlockSpec((1, rows, 1), lambda g, h, *_: (g, 0, 0)),
        ],
        out_specs=pl.BlockSpec((1, rows, per_step * head_size), lambda g, h, *_: (g, 0, h)),
        scratch_shapes=[
            pltpu.VMEM((stacks, stack * rows, 2 * head_size), jnp.float32),
            pltpu.VMEM((stacks, stack * rows, head_size), jnp.float32),
        ],
    )
    return pl.pallas_call(
        kernel,
        grid_spec=spec,
        out_shape=jax.ShapeDtypeStruct((groups, rows, width), jnp.bfloat16),
        compiler_params=pltpu.CompilerParams(vmem_limit_bytes=40 * 2**20),
        cost_estimate=pl.CostEstimate(
            flops=groups * rows * width * tokens * 2,
            bytes_accessed=groups * rows * width * 4,
            transcendentals=groups * rows * heads * tokens // 2,
        ),
    )(low, high, bases, queries, keys, values, starts)


def on_device(
    queries, keys, values, documents, hist_q, hist_kv, out_weight, *, ctx, tp, groups, chunks
):
    rows_here, width = queries.shape
    kv_heads = hist_kv.shape[2]
    heads_here = hist_q.shape[1]
    group = heads_here // kv_heads
    head_size = width // heads_here
    near = ctx // groups
    far_sets = [[g * near + n for g in range(groups)] for n in range(near)]
    near_sets = [[g * near + n for n in range(near)] for g in range(groups)]
    place = lax.axis_index("ctx")
    mine = lax.axis_index("tp")
    far, close = place // near, place % near
    columns = out_weight.shape[1] // tp

    def passed(array, shift):
        return lax.ppermute(array, "tp", [(t, (t + shift) % tp) for t in range(tp)])

    def weight_columns(owner):
        return lax.dynamic_slice_in_dim(out_weight, owner * columns, columns, axis=1)

    query_limit = jnp.max(hist_q, axis=0)
    pair_limit = jnp.max(hist_kv, axis=1)

    def clip(array, limit):
        wide = jnp.repeat(limit, head_size)[None, :]
        return jnp.clip(array.astype(jnp.float32), -wide, wide).astype(jnp.bfloat16)

    leaving = [weight_columns((mine + shift) % tp) for shift in range(tp)]

    def gathered(piece):
        return lax.all_gather(piece, "ctx", axis=0, axis_index_groups=near_sets, tiled=True)

    keys_in, leaving[0] = lax.optimization_barrier((keys, leaving[0]))
    weights = [gathered(leaving[0])]
    arrived = [passed(leaving[shift], shift) for shift in range(1, tp)]
    key_clip, value_clip = clip(keys_in, pair_limit[0]), clip(values, pair_limit[1])
    tokens = documents.shape[0]
    if kv_heads % groups == 0:
        kv_here = kv_heads // groups
        part = kv_here * head_size
        both = jnp.concatenate(
            [key_clip.reshape(rows_here, groups, part), value_clip.reshape(rows_here, groups, part)],
            axis=2,
        )
        both = jnp.transpose(both, (1, 0, 2))
        both = lax.all_to_all(both, "ctx", 0, 0, axis_index_groups=far_sets, tiled=True)
        both, weights[0], *arrived = lax.optimization_barrier((both, weights[0], *arrived))
        both = lax.all_gather(both, "ctx", axis=0, axis_index_groups=near_sets)
        both = jnp.transpose(both, (1, 0, 2, 3)).reshape(tokens, 2 * part)
        key_all, value_all = both[:, :part], both[:, part:]
        kv_first = [j for j in range(kv_here)]
    else:
        kv_here = 1
        both = lax.all_gather(
            jnp.concatenate([key_clip, value_clip], axis=1), "ctx", axis=0, tiled=True
        )
        head = far * (heads_here // groups) // group
        key_all = lax.dynamic_slice_in_dim(both, head * head_size, head_size, axis=1)
        value_all = lax.dynamic_slice_in_dim(
            both, (kv_heads + head) * head_size, head_size, axis=1
        )
        kv_first = [0]
    query_clip = clip(queries, query_limit)
    query_part = width // groups
    query_all = jnp.transpose(query_clip.reshape(rows_here, groups, query_part), (1, 0, 2))
    query_all = lax.all_to_all(query_all, "ctx", 0, 0, axis_index_groups=far_sets, tiled=True)

    weights += [gathered(piece) for piece in arrived]

    rows = rows_here // chunks
    share = query_part // kv_here
    ones = jnp.ones((tokens, head_size), jnp.bfloat16)
    outs = []
    for chunk in range(chunks):
        bases = (jnp.arange(groups, dtype=jnp.int32) * near + close) * rows_here + chunk * rows
        row_pos = bases[:, None] + jnp.arange(rows, dtype=jnp.int32)[None, :]
        row_docs = documents.reshape(groups, near, rows_here)
        row_docs = lax.dynamic_index_in_dim(row_docs, close, 1, keepdims=False)
        row_docs = row_docs[:, chunk * rows : (chunk + 1) * rows]
        starts = jnp.sum(
            (documents[None, None, :] < row_docs[:, :, None]).astype(jnp.int32), axis=2
        )[:, :, None]
        pieces = []
        for j in kv_first:
            own = slice(j * head_size, (j + 1) * head_size)
            pieces.append(
                attend(
                    query_all[:, :, j * share : (j + 1) * share],
                    key_all[:, own],
                    jnp.concatenate([value_all[:, own], ones], axis=1),
                    starts, bases, chunk, rows, head_size,
                )
            )
        attn = pieces[0] if len(pieces) == 1 else jnp.concatenate(pieces, axis=2)
        attn = attn.reshape(groups * rows, query_part)
        total = jnp.dot(attn, weights[0], preferred_element_type=jnp.float32)
        for shift in range(1, tp):
            total = total + jnp.dot(
                passed(attn, shift), weights[shift], preferred_element_type=jnp.float32
            )
        outs.append(
            lax.psum_scatter(
                total.astype(jnp.bfloat16), "ctx", scatter_dimension=0,
                axis_index_groups=far_sets, tiled=True,
            )
        )
    mixed = jnp.concatenate(outs, axis=0)

    def peak(array, heads):
        size = jnp.abs(array.astype(jnp.float32).reshape(rows_here, heads, head_size))
        return jnp.max(size, axis=(0, 2))

    current_query, current_pair = lax.pmax(
        (peak(queries, heads_here), jnp.stack([peak(keys, kv_heads), peak(values, kv_heads)])),
        "ctx",
    )
    new_hist_q = jnp.concatenate([current_query[None], hist_q[:-1]], axis=0)
    new_hist_kv = jnp.concatenate([current_pair[:, None], hist_kv[:, :-1]], axis=1)
    return (mixed, new_hist_q, new_hist_kv)


def solution(mesh):
    ctx, tp = mesh.shape["ctx"], mesh.shape["tp"]
    groups = max(ctx // 4, 1)
    in_specs = (
        P("ctx", "tp"),
        P("ctx", "tp"),
        P("ctx", "tp"),
        P(),
        P(None, "tp"),
        P(None, None, "tp"),
        P(("tp", "ctx"), None),
    )
    out_specs = (P("ctx", "tp"), P(None, "tp"), P(None, None, "tp"))
    body = functools.partial(on_device, ctx=ctx, tp=tp, groups=groups, chunks=2)
    return jax.shard_map(
        body, mesh=mesh, in_specs=in_specs, out_specs=out_specs, check_vma=False
    )
```
